32 devices in a mesh: pb: 4 (over x, core), pq: 8 (over z, y).
Axes of the slice: x: 2, y: 2, z: 4, core: 2. Of those that a mesh axis runs over, the one named last changes fastest.
Arguments:
- chol_vv: bfloat16 [176, 1792, 1792], P('pb', 'pq'), may hold values from -6 to 6
- chol_ov: bfloat16 [176, 256, 1792], P('pb', 'pq'), may hold values from -6 to 6
- chol_oo: bfloat16 [176, 256, 256], P('pb', 'pq'), may hold values from -6 to 6
- chol_vo: bfloat16 [176, 256, 1792], P('pb', None, 'pq'), may hold values from -6 to 6
- amplitudes: bfloat16 [256, 1792], P(None, 'pq'), may hold values from -0.125 to 0.125
Outputs:
- dressed: bfloat16 [176, 256, 1792], P('pb', 'pq')
- fock_ov: float32 [256, 1792], P('pq')
The draws below stay inside these ranges and needn't reach their ends.
All inputs are finite; a program needn't handle non-finite values.
Results may differ from the reference program's by a relative error of at most 0.0081.
Values may be sent and summed in bfloat16 or wider, within the bound.
A program may use at most 128 MiB of HBM per device.

```python
import jax
import jax.numpy as jnp
from jax import lax

NOCC = 256
NVIRT = 1792
QB = 44
NQ = 176
N_PB = 4


def levels(rng, dims, cuts, low, top_value):
    loudness, own = 1.0, jax.random.fold_in(rng, 6)
    for dim, shards_of in cuts:
        heights = jnp.exp(jax.random.uniform(jax.random.fold_in(own, dim), (shards_of,), jnp.float32, low / len(cuts), top_value / len(cuts)))
        loudness = loudness * jnp.repeat(heights, dims[dim] // shards_of).reshape([-1 if axis == dim else 1 for axis in range(len(dims))])
    return loudness


def noise(own_key, dims, spread, bound, split=(), dtype=jnp.bfloat16):
    drawn = jax.random.normal(own_key, dims, jnp.float32) * spread
    if len(split) > 0:
        drawn = levels(own_key, dims, split, -0.22, 0.18) * drawn
    return jnp.clip(drawn, min=-bound, max=bound).astype(dtype)


def setup_inputs(seed: int = 0) -> dict:
    splits = jax.random.split(jax.random.key(seed), 6)
    chol_vv = noise(splits[0], (NQ, NVIRT, NVIRT), 1.0, 6.0, ((0, 4), (1, 8)))
    chol_ov = noise(splits[1], (NQ, NOCC, NVIRT), 1.0, 6.0, ((0, 4), (1, 8)))
    chol_oo = noise(splits[2], (NQ, NOCC, NOCC), 1.0, 6.0, ((0, 4), (1, 8)))
    chol_vo = noise(splits[3], (NQ, NOCC, NVIRT), 1.0, 6.0, ((0, 4), (2, 8)))
    amplitudes = noise(splits[4], (NOCC, NVIRT), NVIRT ** -0.5, 0.125, ((1, 8),))
    return {"chol_vv": chol_vv, "chol_ov": chol_ov, "chol_oo": chol_oo, "chol_vo": chol_vo, "amplitudes": amplitudes}


def reference(chol_vv, chol_ov, chol_oo, chol_vo, amplitudes):
    def one_vector(blocks):
        block_vv, block_ov, block_oo, block_vo = blocks
        lprime = (block_oo.astype(jnp.float32) + jnp.dot(block_ov, amplitudes.T, preferred_element_type=jnp.float32)).astype(jnp.bfloat16)
        direct = jnp.dot(amplitudes, block_vv.T, preferred_element_type=jnp.float32)
        occupied = jnp.dot(lprime.T, amplitudes, preferred_element_type=jnp.float32)
        return (block_vo.astype(jnp.float32) + direct - occupied).astype(jnp.bfloat16)

    dressed = lax.map(one_vector, (chol_vv, chol_ov, chol_oo, chol_vo))
    amps_wide = amplitudes.astype(jnp.float32)

    def one_coulomb(block):
        return 2.0 * jnp.sum(block.astype(jnp.float32) * amps_wide)

    coulomb = lax.map(one_coulomb, dressed)

    def add_vector(total, item):
        weight, block = item
        return total + weight * block.astype(jnp.float32), None

    start = jnp.zeros(amplitudes.shape, jnp.float32)
    total, unused = lax.scan(add_vector, start, (coulomb, dressed))
    fock_ov = total / (QB * N_PB)
    return dressed, fock_ov
```

```python
import functools

import jax
import jax.numpy as jnp
from jax import lax
from jax.experimental import pallas as pl
from jax.experimental.pallas import tpu as pltpu
from jax.sharding import PartitionSpec as P

MESH = pl.DeviceIdType.MESH


def per_device(chol_vv, chol_ov, chol_oo, chol_vo, amplitudes):
    batch = chol_vv.shape[0]
    occ_rows = chol_ov.shape[1]
    whole_amps = lax.all_gather(amplitudes, "pq", axis=1, tiled=True)
    lprime = (
        chol_oo.astype(jnp.float32)
        + jnp.einsum("qjb,ib->qji", chol_ov, whole_amps, preferred_element_type=jnp.float32)
    ).astype(jnp.bfloat16)
    direct = jnp.einsum("qab,ib->qia", chol_vv, whole_amps, preferred_element_type=jnp.float32)
    partial_sum = chol_vo.astype(jnp.float32) + direct
    occupied = jnp.einsum(
        "qji,ja->qia",
        lax.all_gather(lprime, "pq", axis=1, tiled=True),
        amplitudes,
        preferred_element_type=jnp.float32,
    )
    local_dressed = (partial_sum - occupied).astype(jnp.bfloat16)
    dressed = lax.all_to_all(local_dressed, "pq", split_axis=1, concat_axis=2, tiled=True)
    row_start = lax.axis_index("pq") * occ_rows
    own_amps = lax.dynamic_slice_in_dim(whole_amps, row_start, occ_rows, 0)
    local_coulomb = 2.0 * jnp.einsum(
        "qia,ia->q", dressed, own_amps, preferred_element_type=jnp.float32
    )
    coulomb = lax.psum(local_coulomb, "pq")
    local_fock = jnp.sum(coulomb[:, None, None] * dressed.astype(jnp.float32), axis=0)
    fock_ov = lax.psum(local_fock, "pb") / (batch * lax.axis_size("pb"))
    return (dressed, fock_ov)


def kernel(
    n, n_pb, group,
    vv_hbm, ov_hbm, oo_hbm, vo_hbm, amps_hbm,
    dressed, fock_ref,
    vv_buf, ov_buf, oo_buf, vo_buf, amps_t, amps, tiled, gram, occ_buf,
    sent, got, coul_sent, coul_got, part_sent, part_got, sums_sent, sums_got,
    load_sem, own_sem, gather_send, gather_recv, send_sem, recv_sem,
    coul_sem, part_sem, sums_sem, fock_sem,
):
    me = lax.axis_index("pq")
    mine = lax.axis_index("pb")
    batch, virt, whole_virt = vv_hbm.shape
    rows, occ = ov_hbm.shape[1], oo_hbm.shape[2]
    steps = batch // group
    last = steps - 1
    wide, deep = group * virt, group * rows
    span = wide + deep
    sub = rows // n_pb
    half_n = n // 2
    peers = [lax.rem(me + d, n) for d in range(1, n)]
    core, place = lax.rem(mine, 2), mine // 2
    mate, across = mine + 1 - 2 * core, lax.rem(mine + 2, 4)
    partners = [mate, across, lax.rem(mate + 2, 4)]

    barrier = pltpu.get_barrier_semaphore()
    for peer in peers:
        pl.semaphore_signal(barrier, inc=1, device_id={"pq": peer}, device_id_type=MESH)
    for partner in partners:
        pl.semaphore_signal(barrier, inc=1, device_id={"pb": partner}, device_id_type=MESH)

    own_block = pl.ds(pl.multiple_of(me * virt, 16), virt)
    own = pltpu.make_async_copy(amps_hbm, amps_t.at[own_block], own_sem)
    own.start()

    def loads(step, slot):
        part = pl.ds(step * group, group)
        pairs = ((vv_hbm, vv_buf), (ov_hbm, ov_buf), (oo_hbm, oo_buf), (vo_hbm, vo_buf))
        return [
            pltpu.make_async_copy(src.at[part], dst.at[slot], load_sem.at[slot, k])
            for k, (src, dst) in enumerate(pairs)
        ]

    for copy in loads(0, 0):
        copy.start()

    def remote(src, dst, send, recv, where):
        return pltpu.make_async_remote_copy(
            src_ref=src, dst_ref=dst, send_sem=send, recv_sem=recv,
            device_id=where, device_id_type=MESH,
        )

    half_virt, half_occ = virt // 2, occ // 2
    own_columns = pl.ds(pl.multiple_of(core * half_occ, 128), half_occ)

    def quarter(owner):
        first = pl.multiple_of(owner * virt + place * half_virt, 16)
        return amps_t.at[pl.ds(first, half_virt), own_columns]

    side = me // half_n
    spot = lax.rem(me, half_n)
    near = [(1 - side) * half_n + lax.rem(side * (half_n // 2) + k, half_n) for k in range(half_n)]
    home = [side * half_n + lax.rem(spot + d, half_n) for d in range(1, half_n)]
    targets = near[:half_n // 2] + home + near[half_n // 2:]

    def gather(stage, owner, ref, where):
        return remote(ref, ref, gather_send, gather_recv.at[stage, owner], where)

    own.wait()
    pl.semaphore_wait(barrier, len(peers) + len(partners))
    for peer in targets:
        gather(0, me, quarter(me), {"pq": peer}).start()

    def half(owner):
        block = pl.ds(pl.multiple_of(owner * virt, 16), virt)
        return amps_t.at[block, own_columns]

    for owner in home + near:
        gather(0, owner, quarter(owner), {"pq": owner}).wait_recv()
        gather(1, owner, quarter(owner), {"pb": across}).start()

    def turn(owner):
        gather(1, owner, quarter(owner), {"pb": across}).wait_recv()
        gather(2, owner, half(owner), {"pb": mate}).start()

    def close(owner):
        gather(2, owner, half(owner), {"pb": mate}).wait_recv()

    def message(step, d):
        return remote(
            sent.at[step, pl.ds(pl.multiple_of(peers[d] * rows, 16), rows)],
            got.at[step, me],
            send_sem, recv_sem.at[step], {"pq": peers[d]},
        )

    def last_message(d, columns, k):
        return remote(
            sent.at[last, pl.ds(pl.multiple_of(peers[d] * rows, 16), rows), columns],
            got.at[last, me, :, columns],
            send_sem, recv_sem.at[last + k], {"pq": peers[d]},
        )

    def arrived(ref, sem, where):
        remote(ref, ref, send_sem, sem, where).wait_recv()

    direct_columns, lprime_columns = pl.ds(0, wide), pl.ds(wide, deep)
    early, middle = min(last, 3), min(last, 7)

    def form(slot):
        vv = vv_buf[slot].reshape(wide, whole_virt)
        direct = jnp.dot(vv, amps_t[...], preferred_element_type=jnp.float32)
        direct = direct + vo_buf[slot].reshape(wide, occ).astype(jnp.float32)
        ov = ov_buf[slot].reshape(deep, whole_virt)
        lprime = jnp.dot(ov, amps_t[...], preferred_element_type=jnp.float32)
        lprime = lprime + oo_buf[slot].reshape(deep, occ).astype(jnp.float32)
        return direct, lprime

    def put(step, direct, lprime):
        sent[step, :, 0:wide] = direct.T.astype(jnp.bfloat16)
        sent[step, :, wide:span] = lprime.T.astype(jnp.bfloat16)
        got[step, me] = sent[step, pl.ds(pl.multiple_of(me * rows, 16), rows), :]

    def send(step, carry):
        for d in range(n - 1):
            message(step, d).start()
        return carry

    half_whole = whole_virt // 2

    def half_form(which, direct, lprime):
        part = pl.ds(pl.multiple_of(which * half_whole, 128), half_whole)
        block = amps_t[part, :]
        vv = vv_buf[0, :, :, part].reshape(wide, half_whole)
        ov = ov_buf[0, :, :, part].reshape(deep, half_whole)
        direct = direct + jnp.dot(vv, block, preferred_element_type=jnp.float32)
        lprime = lprime + jnp.dot(ov, block, preferred_element_type=jnp.float32)
        return direct, lprime

    for owner in home:
        turn(owner)
    for copy in loads(0, 0):
        copy.wait()
    for owner in home:
        close(owner)
    direct = vo_buf[0].reshape(wide, occ).astype(jnp.float32)
    lprime = oo_buf[0].reshape(deep, occ).astype(jnp.float32)
    direct, lprime = half_form(side, direct, lprime)
    for owner in near:
        turn(owner)
    for owner in near:
        close(owner)
    direct, lprime = half_form(1 - side, direct, lprime)
    put(0, direct, lprime)
    send(0, 0)
    whole_gather = amps_t.at[pl.ds(0, (n - 1) * virt), :]
    remote(whole_gather, whole_gather, gather_send, gather_recv.at[0, me], {"pb": mate}).wait_send()

    for s in range(n):
        block = amps_t[s * virt:(s + 1) * virt, :]
        amps_t_f32 = block.astype(jnp.float32)
        tiled[:, s * virt:(s + 1) * virt] = amps_t_f32.T
    for s in range(n):
        part = tiled[s * rows:(s + 1) * rows, :].astype(jnp.bfloat16)
        for q in range(group):
            amps[s * deep + q * rows:s * deep + (q + 1) * rows, :] = part
    own_rows = amps[pl.ds(pl.multiple_of(me * deep, 128), rows), :]
    gram[...] = jnp.dot(own_rows, amps_t[...], preferred_element_type=jnp.float32)
    coul_sent[...] = jnp.zeros_like(coul_sent)

    def produce(step, carry):
        slot = lax.rem(step, 2)

        @pl.when(step + 1 < steps)
        def _():
            for copy in loads(step + 1, 1 - slot):
                copy.start()

        @pl.when(step > 0)
        def _():
            for copy in loads(step, slot):
                copy.wait()

        direct, lprime = form(slot)

        @pl.when(step > 0)
        def _():
            put(step, direct, lprime)

        own_amps = amps_t[own_block, :].astype(jnp.float32)
        lane = lax.broadcasted_iota(jnp.int32, coul_sent.shape, 1)
        held = coul_sent[...]
        for q in range(group):
            from_direct = direct[q * virt:(q + 1) * virt] * own_amps
            from_occ = lprime[q * rows:(q + 1) * rows] * gram[...]
            value = jnp.sum(from_direct) - jnp.sum(from_occ)
            held = jnp.where(lane == step * group + q, value, held)
        coul_sent[...] = held

        @pl.when((step > 0) & (step < early))
        def _():
            send(step, 0)

        return carry

    lax.fori_loop(0, steps, produce, 0)

    for d in range(n - 1):
        remote(coul_sent, coul_got.at[me], coul_sem.at[0], coul_sem.at[1], {"pq": peers[d]}).start()
    lax.fori_loop(early, middle, send, 0)
    all_coul = coul_got.at[pl.ds(0, n - 1)]
    remote(all_coul, all_coul, coul_sem.at[0], coul_sem.at[1], {"pq": peers[0]}).wait()

    coulomb = coul_sent[...]
    for d in range(n - 1):
        coulomb = coulomb + coul_got[peers[d]]
    lines = -(-steps // 8) * 8
    spread = jnp.broadcast_to(coulomb, (lines, 128))
    lane = lax.broadcasted_iota(jnp.int32, (lines, 128), 1)
    first = lax.broadcasted_iota(jnp.int32, (lines, 128), 0) * group
    spread = jnp.where((lane >= first) & (lane < first + group), spread, 0.0)
    column = lax.broadcasted_iota(jnp.int32, (128, span), 1)
    vector = jnp.zeros((128, span), jnp.int32)
    for q in range(1, group):
        vector = vector + jnp.where((column >= q * virt) & (column < wide), 1, 0)
        vector = vector + jnp.where(column >= wide + q * rows, 1, 0)
    place_of = lax.rem(lax.broadcasted_iota(jnp.int32, (128, span), 0), group)
    pick = jnp.where(place_of == vector, 1.0, 0.0)
    weights = jnp.dot(
        spread, pick, preferred_element_type=jnp.float32, precision=lax.Precision.HIGHEST
    )

    def weigh(d, carry):
        block = pl.ds(pl.multiple_of(d * rows, 16), rows)
        total = jnp.zeros((rows, span), jnp.float32)
        for s in range(steps):
            total = total + weights[s:s + 1, :] * sent[s, block, :].astype(jnp.float32)
        from_direct = total[:, 0:virt]
        from_occ = total[:, wide:wide + rows]
        for q in range(1, group):
            from_direct = from_direct + total[:, q * virt:(q + 1) * virt]
            from_occ = from_occ + total[:, wide + q * rows:wide + (q + 1) * rows]
        total = jnp.concatenate([from_direct, from_occ], axis=1)
        for m in range(n_pb):
            part_sent[m, d] = total[m * sub:(m + 1) * sub]
        return carry

    lax.fori_loop(0, n, weigh, 0)

    for partner in partners:
        remote(
            part_sent.at[partner], part_got.at[mine], part_sem.at[0], part_sem.at[1], {"pb": partner}
        ).start()

    def consume(step, carry):
        @pl.when(step == min(2, last - 1))
        def _():
            three = part_got.at[pl.ds(0, n_pb - 1)]
            remote(three, three, part_sem.at[0], part_sem.at[1], {"pb": mate}).wait()
            total = part_sent[mine]
            for partner in partners:
                total = total + part_got[partner]
            total = total.astype(jnp.bfloat16)
            for s in range(n):
                sums_sent[s] = jnp.concatenate([total[s, :, 0:128], total[s, :, 128:256]], axis=0)
            sums_got[me] = sums_sent[me]
            for d in range(n - 1):
                remote(
                    sums_sent.at[peers[d]], sums_got.at[me], sums_sem.at[0], sums_sem.at[1],
                    {"pq": peers[d]},
                ).start()
            lax.fori_loop(middle, last, send, 0)
            for d in range(n - 1):
                last_message(d, lprime_columns, 0).start()
            for d in range(n - 1):
                last_message(d, direct_columns, 1).start()

        @pl.when(step == last - 1)
        def _():
            several = sums_got.at[pl.ds(0, n - 1)]
            remote(several, several, sums_sem.at[0], sums_sem.at[1], {"pq": peers[0]}).wait()
            pieces = [sums_got[s] for s in range(n)]
            pieces = [
                jnp.concatenate([piece[0:sub], piece[sub:2 * sub]], axis=1).astype(jnp.float32)
                for piece in pieces
            ]
            partial_sum = jnp.concatenate([piece[:, 0:virt] for piece in pieces], axis=1)
            from_occ = jnp.concatenate([piece[:, virt:virt + rows] for piece in pieces], axis=1)
            from_occ = jnp.dot(
                from_occ.astype(jnp.bfloat16), tiled[...].astype(jnp.bfloat16),
                preferred_element_type=jnp.float32,
            )
            strip = pl.ds(pl.multiple_of(mine * sub, 8), sub)
            fock_ref[strip, :] = (partial_sum - from_occ) * (2.0 / (batch * n_pb))
            for partner in partners:
                remote(
                    fock_ref.at[strip], fock_ref.at[strip], fock_sem.at[0], fock_sem.at[1],
                    {"pb": partner},
                ).start()

        arrived(got.at[step, pl.ds(0, n - 1)], recv_sem.at[step], {"pq": peers[0]})
        subtract(step)
        finish(step)
        return carry

    def subtract(step):
        lane_q = lax.broadcasted_iota(jnp.int32, (rows, deep), 1) // rows
        columns = []
        for s in range(n):
            piece = got[step, s, :, wide:span]
            columns.append(jnp.concatenate(
                [jnp.where(lane_q == q, piece, jnp.zeros_like(piece)) for q in range(group)], axis=0
            ))
        occ_buf[...] = jnp.dot(
            jnp.concatenate(columns, axis=1), amps[...], preferred_element_type=jnp.float32
        )

    def finish(step):
        for q in range(group):
            partial_sum = jnp.concatenate(
                [got[step, s, :, q * virt:(q + 1) * virt].astype(jnp.float32) for s in range(n)],
                axis=1,
            )
            value = partial_sum - occ_buf[q * rows:(q + 1) * rows, :]
            dressed[step * group + q] = value.astype(jnp.bfloat16)

    lax.fori_loop(0, last, consume, 0)
    arrived(
        got.at[last, pl.ds(0, n - 1), :, lprime_columns], recv_sem.at[last], {"pq": peers[0]}
    )
    subtract(last)
    strips = fock_ref.at[pl.ds(0, (n_pb - 1) * sub)]
    remote(strips, strips, fock_sem.at[0], fock_sem.at[1], {"pb": mate}).wait()
    arrived(
        got.at[last, pl.ds(0, n - 1), :, direct_columns], recv_sem.at[last + 1], {"pq": peers[0]}
    )
    finish(last)
    everything = sent.at[:, pl.ds(0, (n - 1) * rows), :]
    remote(everything, everything, send_sem, recv_sem.at[0], {"pq": peers[0]}).wait_send()


def fused(n, n_pb, group, chol_vv, chol_ov, chol_oo, chol_vo, amplitudes):
    batch, virt, whole_virt = chol_vv.shape
    rows, occ = chol_ov.shape[1], chol_oo.shape[2]
    steps = batch // group
    wide, deep = group * virt, group * rows
    sub = rows // n_pb
    bf16, f32 = jnp.bfloat16, jnp.float32
    dma = pltpu.SemaphoreType.DMA
    whole = pl.BlockSpec(memory_space=pltpu.VMEM)
    hbm = pl.BlockSpec(memory_space=pl.ANY)
    return pl.pallas_call(
        functools.partial(kernel, n, n_pb, group),
        out_shape=(
            pltpu.VMEM((batch, rows, whole_virt), bf16),
            pltpu.VMEM((rows, whole_virt), f32),
        ),
        in_specs=[hbm, hbm, hbm, hbm, hbm],
        out_specs=(whole, whole),
        scratch_shapes=[
            pltpu.VMEM((2, group, virt, whole_virt), bf16),
            pltpu.VMEM((2, group, rows, whole_virt), bf16),
            pltpu.VMEM((2, group, rows, occ), bf16),
            pltpu.VMEM((2, group, virt, occ), bf16),
            pltpu.VMEM((whole_virt, occ), bf16),
            pltpu.VMEM((n * deep, whole_virt), bf16),
            pltpu.VMEM((occ, whole_virt), f32),
            pltpu.VMEM((rows, occ), f32),
            pltpu.VMEM((deep, whole_virt), f32),
            pltpu.VMEM((steps, occ, wide + deep), bf16),
            pltpu.VMEM((steps, n, rows, wide + deep), bf16),
            pltpu.VMEM((1, 128), f32),
            pltpu.VMEM((n, 1, 128), f32),
            pltpu.VMEM((n_pb, n, sub, virt + rows), f32),
            pltpu.VMEM((n_pb, n, sub, virt + rows), f32),
            pltpu.VMEM((n, 2 * sub, 128), bf16),
            pltpu.VMEM((n, 2 * sub, 128), bf16),
            dma((2, 4)), dma, dma, dma((3, n)), dma, dma((steps + 1,)),
            dma((2,)), dma((2,)), dma((2,)), dma((2,)),
        ],
        compiler_params=pltpu.CompilerParams(
            collective_id=0, has_side_effects=True, vmem_limit_bytes=59800 * 1024
        ),
    )(chol_vv, chol_ov, chol_oo, jnp.swapaxes(chol_vo, 1, 2), amplitudes.T)


def group_size(batch, virt, rows):
    for group in range(1, batch + 1):
        if batch % group == 0 and group * virt % 128 == 0 and group * rows % 128 == 0:
            return group
    return None


def solution(mesh):
    n, n_pb = mesh.shape["pq"], mesh.shape["pb"]
    in_specs = (
        P("pb", "pq", None),
        P("pb", "pq", None),
        P("pb", "pq", None),
        P("pb", None, "pq"),
        P(None, "pq"),
    )
    out_specs = (P("pb", "pq", None), P("pq", None))

    def body(chol_vv, chol_ov, chol_oo, chol_vo, amplitudes):
        batch, virt, whole_virt = chol_vv.shape
        rows, occ = chol_ov.shape[1], chol_oo.shape[2]
        group = group_size(batch, virt, rows)
        fits = group is not None and group <= 8 and virt % 32 == 0 and rows % 16 == 0
        fits = fits and occ % 256 == 0 and n_pb == 4 and n > 1 and n % 4 == 0
        fits = fits and virt + rows == 256 and rows == 8 * n_pb and 3 <= batch // group <= 16
        fits = fits and batch <= 128 and whole_virt % 256 == 0
        if fits:
            return fused(n, n_pb, group, chol_vv, chol_ov, chol_oo, chol_vo, amplitudes)
        return per_device(chol_vv, chol_ov, chol_oo, chol_vo, amplitudes)

    return jax.shard_map(
        body, mesh=mesh, in_specs=in_specs, out_specs=out_specs, check_vma=False
    )
```

```python
import functools

import jax
import jax.numpy as jnp
from jax import lax
from jax.experimental import pallas as pl
from jax.experimental.pallas import tpu as pltpu
from jax.sharding import PartitionSpec as P

MESH = pl.DeviceIdType.MESH


def per_device(chol_vv, chol_ov, chol_oo, chol_vo, amplitudes):
    batch = chol_vv.shape[0]
    occ_rows = chol_ov.shape[1]
    whole_amps = lax.all_gather(amplitudes, "pq", axis=1, tiled=True)
    lprime = (
        chol_oo.astype(jnp.float32)
        + jnp.einsum("qjb,ib->qji", chol_ov, whole_amps, preferred_element_type=jnp.float32)
    ).astype(jnp.bfloat16)
    direct = jnp.einsum("qab,ib->qia", chol_vv, whole_amps, preferred_element_type=jnp.float32)
    partial_sum = chol_vo.astype(jnp.float32) + direct
    occupied = jnp.einsum(
        "qji,ja->qia",
        lax.all_gather(lprime, "pq", axis=1, tiled=True),
        amplitudes,
        preferred_element_type=jnp.float32,
    )
    local_dressed = (partial_sum - occupied).astype(jnp.bfloat16)
    dressed = lax.all_to_all(local_dressed, "pq", split_axis=1, concat_axis=2, tiled=True)
    row_start = lax.axis_index("pq") * occ_rows
    own_amps = lax.dynamic_slice_in_dim(whole_amps, row_start, occ_rows, 0)
    local_coulomb = 2.0 * jnp.einsum(
        "qia,ia->q", dressed, own_amps, preferred_element_type=jnp.float32
    )
    coulomb = lax.psum(local_coulomb, "pq")
    local_fock = jnp.sum(coulomb[:, None, None] * dressed.astype(jnp.float32), axis=0)
    fock_ov = lax.psum(local_fock, "pb") / (batch * lax.axis_size("pb"))
    return (dressed, fock_ov)


def kernel(
    n, n_pb, group,
    vv_hbm, ov_hbm, oo_hbm, vo_hbm, amps_hbm,
    dressed, fock_ref,
    vv_buf, ov_buf, oo_buf, vo_buf, amps_t, amps, tiled, gram, occ_buf,
    sent, got, coul_sent, coul_got, part_sent, part_got, sums_sent, sums_got,
    load_sem, own_sem, gather_send, gather_recv, send_sem, recv_sem,
    coul_sem, part_sem, sums_sem, fock_sem, ready,
):
    me = lax.axis_index("pq")
    mine = lax.axis_index("pb")
    batch, virt, whole_virt = vv_hbm.shape
    rows, occ = ov_hbm.shape[1], oo_hbm.shape[2]
    steps = batch // group
    last = steps - 1
    wide, deep = group * virt, group * rows
    span = wide + deep
    sub = rows // n_pb
    half_n, quarter_n = n // 2, n // 4
    peers = [lax.rem(me + d, n) for d in range(1, n)]
    core = lax.rem(mine, 2)
    mate, across = mine + 1 - 2 * core, lax.rem(mine + 2, 4)
    partners = [mate, across, lax.rem(mate + 2, 4)]

    barrier = pltpu.get_barrier_semaphore()
    for peer in peers:
        @pl.when(peer > me)
        def _():
            pl.semaphore_signal(barrier, inc=1, device_id={"pq": peer}, device_id_type=MESH)
    for partner in partners:
        @pl.when(partner > mine)
        def _():
            pl.semaphore_signal(barrier, inc=1, device_id={"pb": partner}, device_id_type=MESH)

    own_block = pl.ds(pl.multiple_of(me * virt, 16), virt)
    own = pltpu.make_async_copy(amps_hbm, amps_t.at[own_block], own_sem)
    own.start()

    def loads(step, slot):
        part = pl.ds(step * group, group)
        pairs = ((vv_hbm, vv_buf), (ov_hbm, ov_buf), (oo_hbm, oo_buf), (vo_hbm, vo_buf))
        return [
            pltpu.make_async_copy(src.at[part], dst.at[slot], load_sem.at[slot, k])
            for k, (src, dst) in enumerate(pairs)
        ]

    for copy in loads(0, 0):
        copy.start()

    def remote(src, dst, send, recv, where):
        return pltpu.make_async_remote_copy(
            src_ref=src, dst_ref=dst, send_sem=send, recv_sem=recv,
            device_id=where, device_id_type=MESH,
        )

    half_virt, half_occ = virt // 2, occ // 2
    side, spot = me // half_n, lax.rem(me, half_n)
    other = 1 - side
    home = [side * half_n + lax.rem(spot + d, half_n) for d in range(1, half_n)]
    cross = [other * half_n + lax.rem(side * quarter_n + k, half_n) for k in range(half_n)]
    near = [cross[0] + lax.rem(spot + k, quarter_n) for k in range(quarter_n)]
    targets = [
        side * second + other * first for first, second in zip(home + near, near + home)
    ]
    is_near = spot // quarter_n == other
    beyond = lax.rem(me + n + quarter_n * (2 * side - 1), n)

    @pl.when(me + mine > 0)
    def _():
        pl.semaphore_wait(barrier, me + mine)

    for peer in peers:
        @pl.when(peer < me)
        def _():
            pl.semaphore_signal(ready.at[me], inc=1, device_id={"pq": peer}, device_id_type=MESH)
    for partner in partners:
        @pl.when(partner < mine)
        def _():
            pl.semaphore_signal(
                ready.at[n + mine], inc=1, device_id={"pb": partner}, device_id_type=MESH
            )

    def greet(peer):
        @pl.when(peer > me)
        def _():
            pl.semaphore_wait(ready.at[peer], 1)

    def greet_partner(partner):
        @pl.when(partner > mine)
        def _():
            pl.semaphore_wait(ready.at[n + partner], 1)

    def columns_of(which):
        return pl.ds(pl.multiple_of(which * half_occ, 128), half_occ)

    def piece(owner, which):
        first = pl.multiple_of(owner * virt + core * half_virt, 16)
        return amps_t.at[pl.ds(first, half_virt), columns_of(which)]

    def hop(owner, turn, which, peer):
        ref = piece(owner, which)
        return remote(ref, ref, gather_send, gather_recv.at[turn, owner], {"pq": peer})

    def swap(owner, turn):
        ref = piece(owner, turns[turn])
        return remote(ref, ref, gather_send, gather_recv.at[2 + turn, owner], {"pb": mate})

    turns = [other, side]
    own.wait()
    for peer in targets:
        greet(peer)
        hop(me, 0, 1 - peer // half_n, peer).start()
    for peer in targets:
        hop(me, 1, peer // half_n, peer).start()

    def pass_on(owners, turn, relay):
        for owner in owners:
            hop(owner, turn, turns[turn], owner).wait_recv()
            if relay:
                @pl.when(is_near)
                def _():
                    hop(owner, turn, turns[turn], beyond).start()
            swap(owner, turn).start()

    def close(owners, turn):
        for owner in owners:
            swap(owner, turn).wait_recv()

    def message(step, peer):
        return remote(
            sent.at[step, pl.ds(pl.multiple_of(peer * rows, 16), rows)],
            got.at[step, me],
            send_sem, recv_sem.at[step], {"pq": peer},
        )

    def last_message(d, columns, k):
        return remote(
            sent.at[last, pl.ds(pl.multiple_of(peers[d] * rows, 16), rows), columns],
            got.at[last, me, :, columns],
            send_sem, recv_sem.at[last + k], {"pq": peers[d]},
        )

    def arrived(ref, sem, where):
        remote(ref, ref, send_sem, sem, where).wait_recv()

    direct_columns, lprime_columns = pl.ds(0, wide), pl.ds(wide, deep)
    early, middle = min(last, 3), min(last, 7)

    def form(slot):
        vv = vv_buf[slot].reshape(wide, whole_virt)
        direct = jnp.dot(vv, amps_t[...], preferred_element_type=jnp.float32)
        direct = direct + vo_buf[slot].reshape(wide, occ).astype(jnp.float32)
        ov = ov_buf[slot].reshape(deep, whole_virt)
        lprime = jnp.dot(ov, amps_t[...], preferred_element_type=jnp.float32)
        lprime = lprime + oo_buf[slot].reshape(deep, occ).astype(jnp.float32)
        return direct, lprime

    def put(step, direct, lprime):
        sent[step, :, 0:wide] = direct.T.astype(jnp.bfloat16)
        sent[step, :, wide:span] = lprime.T.astype(jnp.bfloat16)
        got[step, me] = sent[step, pl.ds(pl.multiple_of(me * rows, 16), rows), :]

    def send(step, carry):
        for peer in peers:
            message(step, peer).start()
        return carry

    half_whole = whole_virt // 2

    def half_form(part, which, direct, lprime):
        part = pl.ds(pl.multiple_of(part * half_whole, 128), half_whole)
        block = amps_t[part, columns_of(which)]
        vv = vv_buf[0, :, :, part].reshape(wide, half_whole)
        ov = ov_buf[0, :, :, part].reshape(deep, half_whole)
        direct = direct + jnp.dot(vv, block, preferred_element_type=jnp.float32)
        lprime = lprime + jnp.dot(ov, block, preferred_element_type=jnp.float32)
        return direct, lprime

    def start_form(which):
        direct = vo_buf[0, :, :, columns_of(which)].reshape(wide, half_occ).astype(jnp.float32)
        lprime = oo_buf[0, :, :, columns_of(which)].reshape(deep, half_occ).astype(jnp.float32)
        return half_form(side, which, direct, lprime)

    def put_half(which, direct, lprime):
        sent[0, columns_of(which), 0:wide] = direct.T.astype(jnp.bfloat16)
        sent[0, columns_of(which), wide:span] = lprime.T.astype(jnp.bfloat16)

    greet_partner(mate)
    pass_on(home, 0, False)
    for copy in loads(0, 0):
        copy.wait()
    close(home, 0)
    direct, lprime = start_form(other)

    pass_on(cross, 0, True)
    close(cross, 0)
    direct, lprime = half_form(other, other, direct, lprime)
    put_half(other, direct, lprime)
    for peer in cross[quarter_n:]:
        greet(peer)
    for peer in cross:
        message(0, peer).start()
    pass_on(home, 1, False)
    pass_on(cross, 1, True)
    close(home + cross, 1)
    direct, lprime = start_form(side)
    direct, lprime = half_form(other, side, direct, lprime)
    put_half(side, direct, lprime)
    got[0, me] = sent[0, pl.ds(pl.multiple_of(me * rows, 16), rows), :]
    for peer in home:
        message(0, peer).start()
    for partner in partners[1:]:
        greet_partner(partner)

    @pl.when(is_near)
    def _():
        ref = amps_t
        remote(ref, ref, gather_send, gather_recv.at[0, me], {"pb": mate}).wait_send()

    @pl.when(jnp.logical_not(is_near))
    def _():
        ref = amps_t.at[pl.ds(0, (n - 2) * virt), :]
        remote(ref, ref, gather_send, gather_recv.at[0, me], {"pb": mate}).wait_send()

    for s in range(n):
        block = amps_t[s * virt:(s + 1) * virt, :]
        amps_t_f32 = block.astype(jnp.float32)
        tiled[:, s * virt:(s + 1) * virt] = amps_t_f32.T
    for s in range(n):
        part = tiled[s * rows:(s + 1) * rows, :].astype(jnp.bfloat16)
        for q in range(group):
            amps[s * deep + q * rows:s * deep + (q + 1) * rows, :] = part
    own_rows = amps[pl.ds(pl.multiple_of(me * deep, 128), rows), :]
    gram[...] = jnp.dot(own_rows, amps_t[...], preferred_element_type=jnp.float32)
    coul_sent[...] = jnp.zeros_like(coul_sent)

    def produce(step, carry):
        slot = lax.rem(step, 2)

        @pl.when(step + 1 < steps)
        def _():
            for copy in loads(step + 1, 1 - slot):
                copy.start()

        @pl.when(step > 0)
        def _():
            for copy in loads(step, slot):
                copy.wait()

        direct, lprime = form(slot)

        @pl.when(step > 0)
        def _():
            put(step, direct, lprime)

        own_amps = amps_t[own_block, :].astype(jnp.float32)
        lane = lax.broadcasted_iota(jnp.int32, coul_sent.shape, 1)
        held = coul_sent[...]
        for q in range(group):
            from_direct = direct[q * virt:(q + 1) * virt] * own_amps
            from_occ = lprime[q * rows:(q + 1) * rows] * gram[...]
            value = jnp.sum(from_direct) - jnp.sum(from_occ)
            held = jnp.where(lane == step * group + q, value, held)
        coul_sent[...] = held

        @pl.when((step > 0) & (step < early))
        def _():
            send(step, 0)

        return carry

    lax.fori_loop(0, steps, produce, 0)

    for d in range(n - 1):
        remote(coul_sent, coul_got.at[me], coul_sem.at[0], coul_sem.at[1], {"pq": peers[d]}).start()
    lax.fori_loop(early, middle, send, 0)
    all_coul = coul_got.at[pl.ds(0, n - 1)]
    remote(all_coul, all_coul, coul_sem.at[0], coul_sem.at[1], {"pq": peers[0]}).wait()

    coulomb = coul_sent[...]
    for d in range(n - 1):
        coulomb = coulomb + coul_got[peers[d]]
    lines = -(-steps // 8) * 8
    spread = jnp.broadcast_to(coulomb, (lines, 128))
    lane = lax.broadcasted_iota(jnp.int32, (lines, 128), 1)
    first = lax.broadcasted_iota(jnp.int32, (lines, 128), 0) * group
    spread = jnp.where((lane >= first) & (lane < first + group), spread, 0.0)
    column = lax.broadcasted_iota(jnp.int32, (128, span), 1)
    vector = jnp.zeros((128, span), jnp.int32)
    for q in range(1, group):
        vector = vector + jnp.where((column >= q * virt) & (column < wide), 1, 0)
        vector = vector + jnp.where(column >= wide + q * rows, 1, 0)
    place_of = lax.rem(lax.broadcasted_iota(jnp.int32, (128, span), 0), group)
    pick = jnp.where(place_of == vector, 1.0, 0.0)
    weights = jnp.dot(
        spread, pick, preferred_element_type=jnp.float32, precision=lax.Precision.HIGHEST
    )

    def weigh(d, carry):
        block = pl.ds(pl.multiple_of(d * rows, 16), rows)
        total = jnp.zeros((rows, span), jnp.float32)
        for s in range(steps):
            total = total + weights[s:s + 1, :] * sent[s, block, :].astype(jnp.float32)
        from_direct = total[:, 0:virt]
        from_occ = total[:, wide:wide + rows]
        for q in range(1, group):
            from_direct = from_direct + total[:, q * virt:(q + 1) * virt]
            from_occ = from_occ + total[:, wide + q * rows:wide + (q + 1) * rows]
        total = jnp.concatenate([from_direct, from_occ], axis=1)
        for m in range(n_pb):
            part_sent[m, d] = total[m * sub:(m + 1) * sub]
        return carry

    lax.fori_loop(0, n, weigh, 0)

    for partner in partners:
        remote(
            part_sent.at[partner], part_got.at[mine], part_sem.at[0], part_sem.at[1], {"pb": partner}
        ).start()

    def consume(step, carry):
        @pl.when(step == min(2, last - 1))
        def _():
            three = part_got.at[pl.ds(0, n_pb - 1)]
            remote(three, three, part_sem.at[0], part_sem.at[1], {"pb": mate}).wait()
            total = part_sent[mine]
            for partner in partners:
                total = total + part_got[partner]
            total = total.astype(jnp.bfloat16)
            for s in range(n):
                sums_sent[s] = jnp.concatenate([total[s, :, 0:128], total[s, :, 128:256]], axis=0)
            sums_got[me] = sums_sent[me]
            for d in range(n - 1):
                remote(
                    sums_sent.at[peers[d]], sums_got.at[me], sums_sem.at[0], sums_sem.at[1],
                    {"pq": peers[d]},
                ).start()
            lax.fori_loop(middle, last, send, 0)
            for d in range(n - 1):
                last_message(d, lprime_columns, 0).start()
            for d in range(n - 1):
                last_message(d, direct_columns, 1).start()

        @pl.when(step == last - 1)
        def _():
            several = sums_got.at[pl.ds(0, n - 1)]
            remote(several, several, sums_sem.at[0], sums_sem.at[1], {"pq": peers[0]}).wait()
            pieces = [sums_got[s] for s in range(n)]
            pieces = [
                jnp.concatenate([piece[0:sub], piece[sub:2 * sub]], axis=1).astype(jnp.float32)
                for piece in pieces
            ]
            partial_sum = jnp.concatenate([piece[:, 0:virt] for piece in pieces], axis=1)
            from_occ = jnp.concatenate([piece[:, virt:virt + rows] for piece in pieces], axis=1)
            from_occ = jnp.dot(
                from_occ.astype(jnp.bfloat16), tiled[...].astype(jnp.bfloat16),
                preferred_element_type=jnp.float32,
            )
            strip = pl.ds(pl.multiple_of(mine * sub, 8), sub)
            fock_ref[strip, :] = (partial_sum - from_occ) * (2.0 / (batch * n_pb))
            for partner in partners:
                remote(
                    fock_ref.at[strip], fock_ref.at[strip], fock_sem.at[0], fock_sem.at[1],
                    {"pb": partner},
                ).start()

        arrived(got.at[step, pl.ds(0, n - 1)], recv_sem.at[step], {"pq": peers[0]})
        subtract(step)
        finish(step)
        return carry

    def subtract(step):
        lane_q = lax.broadcasted_iota(jnp.int32, (rows, deep), 1) // rows
        columns = []
        for s in range(n):
            piece = got[step, s, :, wide:span]
            columns.append(jnp.concatenate(
                [jnp.where(lane_q == q, piece, jnp.zeros_like(piece)) for q in range(group)], axis=0
            ))
        occ_buf[...] = jnp.dot(
            jnp.concatenate(columns, axis=1), amps[...], preferred_element_type=jnp.float32
        )

    def finish(step):
        for q in range(group):
            partial_sum = jnp.concatenate(
                [got[step, s, :, q * virt:(q + 1) * virt].astype(jnp.float32) for s in range(n)],
                axis=1,
            )
            value = partial_sum - occ_buf[q * rows:(q + 1) * rows, :]
            dressed[step * group + q] = value.astype(jnp.bfloat16)

    lax.fori_loop(0, last, consume, 0)
    arrived(
        got.at[last, pl.ds(0, n - 1), :, lprime_columns], recv_sem.at[last], {"pq": peers[0]}
    )
    subtract(last)
    strips = fock_ref.at[pl.ds(0, (n_pb - 1) * sub)]
    remote(strips, strips, fock_sem.at[0], fock_sem.at[1], {"pb": mate}).wait()
    arrived(
        got.at[last, pl.ds(0, n - 1), :, direct_columns], recv_sem.at[last + 1], {"pq": peers[0]}
    )
    finish(last)
    everything = sent.at[:, pl.ds(0, (n - 1) * rows), :]
    remote(everything, everything, send_sem, recv_sem.at[0], {"pq": peers[0]}).wait_send()


def fused(n, n_pb, group, chol_vv, chol_ov, chol_oo, chol_vo, amplitudes):
    batch, virt, whole_virt = chol_vv.shape
    rows, occ = chol_ov.shape[1], chol_oo.shape[2]
    steps = batch // group
    wide, deep = group * virt, group * rows
    sub = rows // n_pb
    bf16, f32 = jnp.bfloat16, jnp.float32
    dma = pltpu.SemaphoreType.DMA
    whole = pl.BlockSpec(memory_space=pltpu.VMEM)
    hbm = pl.BlockSpec(memory_space=pl.ANY)
    return pl.pallas_call(
        functools.partial(kernel, n, n_pb, group),
        out_shape=(
            pltpu.VMEM((batch, rows, whole_virt), bf16),
            pltpu.VMEM((rows, whole_virt), f32),
        ),
        in_specs=[hbm, hbm, hbm, hbm, hbm],
        out_specs=(whole, whole),
        scratch_shapes=[
            pltpu.VMEM((2, group, virt, whole_virt), bf16),
            pltpu.VMEM((2, group, rows, whole_virt), bf16),
            pltpu.VMEM((2, group, rows, occ), bf16),
            pltpu.VMEM((2, group, virt, occ), bf16),
            pltpu.VMEM((whole_virt, occ), bf16),
            pltpu.VMEM((n * deep, whole_virt), bf16),
            pltpu.VMEM((occ, whole_virt), f32),
            pltpu.VMEM((rows, occ), f32),
            pltpu.VMEM((deep, whole_virt), f32),
            pltpu.VMEM((steps, occ, wide + deep), bf16),
            pltpu.VMEM((steps, n, rows, wide + deep), bf16),
            pltpu.VMEM((1, 128), f32),
            pltpu.VMEM((n, 1, 128), f32),
            pltpu.VMEM((n_pb, n, sub, virt + rows), f32),
            pltpu.VMEM((n_pb, n, sub, virt + rows), f32),
            pltpu.VMEM((n, 2 * sub, 128), bf16),
            pltpu.VMEM((n, 2 * sub, 128), bf16),
            dma((2, 4)), dma, dma, dma((4, n)), dma, dma((steps + 1,)),
            dma((2,)), dma((2,)), dma((2,)), dma((2,)),
            pltpu.SemaphoreType.REGULAR((n + n_pb,)),
        ],
        compiler_params=pltpu.CompilerParams(
            collective_id=0, has_side_effects=True, vmem_limit_bytes=59800 * 1024
        ),
    )(chol_vv, chol_ov, chol_oo, jnp.swapaxes(chol_vo, 1, 2), amplitudes.T)


def group_size(batch, virt, rows):
    for group in range(1, batch + 1):
        if batch % group == 0 and group * virt % 128 == 0 and group * rows % 128 == 0:
            return group
    return None


def solution(mesh):
    n, n_pb = mesh.shape["pq"], mesh.shape["pb"]
    in_specs = (
        P("pb", "pq", None),
        P("pb", "pq", None),
        P("pb", "pq", None),
        P("pb", None, "pq"),
        P(None, "pq"),
    )
    out_specs = (P("pb", "pq", None), P("pq", None))

    def body(chol_vv, chol_ov, chol_oo, chol_vo, amplitudes):
        batch, virt, whole_virt = chol_vv.shape
        rows, occ = chol_ov.shape[1], chol_oo.shape[2]
        group = group_size(batch, virt, rows)
        fits = group is not None and group <= 8 and virt % 32 == 0 and rows % 16 == 0
        fits = fits and occ % 256 == 0 and n_pb == 4 and n == 8
        fits = fits and virt + rows == 256 and rows == 8 * n_pb and 3 <= batch // group <= 16
        fits = fits and batch <= 128 and whole_virt % 256 == 0
        if fits:
            return fused(n, n_pb, group, chol_vv, chol_ov, chol_oo, chol_vo, amplitudes)
        return per_device(chol_vv, chol_ov, chol_oo, chol_vo, amplitudes)

    return jax.shard_map(
        body, mesh=mesh, in_specs=in_specs, out_specs=out_specs, check_vma=False
    )
```

```python
import functools

import jax
import jax.numpy as jnp
from jax import lax
from jax.experimental import pallas as pl
from jax.experimental.pallas import tpu as pltpu
from jax.sharding import PartitionSpec as P

MESH = pl.DeviceIdType.MESH


def per_device(chol_vv, chol_ov, chol_oo, chol_vo, amplitudes):
    batch = chol_vv.shape[0]
    occ_rows = chol_ov.shape[1]
    whole_amps = lax.all_gather(amplitudes, "pq", axis=1, tiled=True)
    lprime = (
        chol_oo.astype(jnp.float32)
        + jnp.einsum("qjb,ib->qji", chol_ov, whole_amps, preferred_element_type=jnp.float32)
    ).astype(jnp.bfloat16)
    direct = jnp.einsum("qab,ib->qia", chol_vv, whole_amps, preferred_element_type=jnp.float32)
    partial_sum = chol_vo.astype(jnp.float32) + direct
    occupied = jnp.einsum(
        "qji,ja->qia",
        lax.all_gather(lprime, "pq", axis=1, tiled=True),
        amplitudes,
        preferred_element_type=jnp.float32,
    )
    local_dressed = (partial_sum - occupied).astype(jnp.bfloat16)
    dressed = lax.all_to_all(local_dressed, "pq", split_axis=1, concat_axis=2, tiled=True)
    row_start = lax.axis_index("pq") * occ_rows
    own_amps = lax.dynamic_slice_in_dim(whole_amps, row_start, occ_rows, 0)
    local_coulomb = 2.0 * jnp.einsum(
        "qia,ia->q", dressed, own_amps, preferred_element_type=jnp.float32
    )
    coulomb = lax.psum(local_coulomb, "pq")
    local_fock = jnp.sum(coulomb[:, None, None] * dressed.astype(jnp.float32), axis=0)
    fock_ov = lax.psum(local_fock, "pb") / (batch * lax.axis_size("pb"))
    return (dressed, fock_ov)


def kernel(
    n, n_pb, group,
    vv_hbm, ov_hbm, oo_hbm, vo_hbm, amps_hbm,
    dressed, fock_ref, got, occ_buf,
    vv_buf, ov_buf, oo_buf, vo_buf, amps_t, amps, tiled, gram,
    sent, coul_sent, coul_got, part_sent, part_got, sums_sent, sums_got,
    load_sem, own_sem, gather_send, gather_recv, send_sem, recv_sem,
    coul_sem, part_sem, sums_sem, fock_sem, ready,
):
    me = lax.axis_index("pq")
    mine = lax.axis_index("pb")
    batch, virt, whole_virt = vv_hbm.shape
    rows, occ = ov_hbm.shape[1], oo_hbm.shape[2]
    steps = batch // group
    last = steps - 1
    wide, deep = group * virt, group * rows
    span = wide + deep
    sub = rows // n_pb
    half_n, quarter_n = n // 2, n // 4
    peers = [lax.rem(me + d, n) for d in range(1, n)]
    core = lax.rem(mine, 2)
    mate, across = mine + 1 - 2 * core, lax.rem(mine + 2, 4)
    partners = [mate, across, lax.rem(mate + 2, 4)]

    barrier = pltpu.get_barrier_semaphore()
    for peer in peers:
        @pl.when(peer > me)
        def _():
            pl.semaphore_signal(barrier, inc=1, device_id={"pq": peer}, device_id_type=MESH)
    for partner in partners:
        @pl.when(partner > mine)
        def _():
            pl.semaphore_signal(barrier, inc=1, device_id={"pb": partner}, device_id_type=MESH)

    own_block = pl.ds(pl.multiple_of(me * virt, 16), virt)
    own = pltpu.make_async_copy(amps_hbm, amps_t.at[own_block], own_sem)
    own.start()

    def loads(step, slot):
        part = pl.ds(step * group, group)
        pairs = ((vv_hbm, vv_buf), (ov_hbm, ov_buf), (oo_hbm, oo_buf), (vo_hbm, vo_buf))
        return [
            pltpu.make_async_copy(src.at[part], dst.at[slot], load_sem.at[slot, k])
            for k, (src, dst) in enumerate(pairs)
        ]

    def remote(src, dst, send, recv, where):
        return pltpu.make_async_remote_copy(
            src_ref=src, dst_ref=dst, send_sem=send, recv_sem=recv,
            device_id=where, device_id_type=MESH,
        )

    half_virt, half_occ = virt // 2, occ // 2
    side, spot = me // half_n, lax.rem(me, half_n)
    other = 1 - side
    home = [side * half_n + lax.rem(spot + d, half_n) for d in range(1, half_n)]
    cross = [other * half_n + lax.rem(side * quarter_n + k, half_n) for k in range(half_n)]
    near = [cross[0] + lax.rem(spot + k, quarter_n) for k in range(quarter_n)]
    targets = [
        second for first, second in zip(home + near, near + home)
    ]
    is_near = spot // quarter_n == other
    beyond = lax.rem(me + n + quarter_n * (2 * side - 1), n)

    @pl.when(me + mine > 0)
    def _():
        pl.semaphore_wait(barrier, me + mine)

    for peer in peers:
        @pl.when(peer < me)
        def _():
            pl.semaphore_signal(ready.at[me], inc=1, device_id={"pq": peer}, device_id_type=MESH)
    for partner in partners:
        @pl.when(partner < mine)
        def _():
            pl.semaphore_signal(
                ready.at[n + mine], inc=1, device_id={"pb": partner}, device_id_type=MESH
            )

    def greet(peer):
        @pl.when(peer > me)
        def _():
            pl.semaphore_wait(ready.at[peer], 1)

    def greet_partner(partner):
        @pl.when(partner > mine)
        def _():
            pl.semaphore_wait(ready.at[n + partner], 1)

    def columns_of(which):
        return pl.ds(pl.multiple_of(which * half_occ, 128), half_occ)

    def piece(owner, which):
        first = pl.multiple_of(owner * virt + core * half_virt, 16)
        return amps_t.at[pl.ds(first, half_virt), columns_of(which)]

    def hop(owner, turn, which, peer):
        ref = piece(owner, which)
        return remote(ref, ref, gather_send, gather_recv.at[turn, owner], {"pq": peer})

    def swap(owner, turn):
        ref = piece(owner, turns[turn])
        return remote(ref, ref, gather_send, gather_recv.at[2 + turn, owner], {"pb": mate})

    turns = [other, side]
    own.wait()
    for peer in targets:
        greet(peer)
        hop(me, 0, 1 - peer // half_n, peer).start()
    for copy in loads(0, 0):
        copy.start()

    def pass_on(owners, turn, relay):
        for owner in owners:
            hop(owner, turn, turns[turn], owner).wait_recv()
            if relay:
                @pl.when(is_near)
                def _():
                    hop(owner, turn, turns[turn], beyond).start()
            swap(owner, turn).start()

    def close(owners, turn):
        for owner in owners:
            swap(owner, turn).wait_recv()

    early, middle = min(last, 3), min(last, 7)
    chunks = [(step, 1) for step in range(early)]
    chunks += [(step, 1) for step in range(early, last)]
    chunks = [(first, count) for first, count in chunks if count > 0]

    def message(k, peer):
        first, count = chunks[k]
        return remote(
            sent.at[peer, pl.ds(first, count)], got.at[me, pl.ds(first, count)],
            send_sem, recv_sem.at[k], {"pq": peer},
        )

    def last_message(peer, columns, k):
        return remote(
            sent.at[peer, last, :, columns], got.at[me, last, :, columns],
            send_sem, recv_sem.at[len(chunks) + k], {"pq": peer},
        )

    def arrived(ref, sem, where):
        remote(ref, ref, send_sem, sem, where).wait_recv()

    direct_columns, lprime_columns = pl.ds(0, wide), pl.ds(wide, deep)

    def form(slot):
        vv = vv_buf[slot].reshape(wide, whole_virt)
        direct = jnp.dot(vv, amps_t[...], preferred_element_type=jnp.float32)
        direct = direct + vo_buf[slot].reshape(wide, occ).astype(jnp.float32)
        ov = ov_buf[slot].reshape(deep, whole_virt)
        lprime = jnp.dot(ov, amps_t[...], preferred_element_type=jnp.float32)
        lprime = lprime + oo_buf[slot].reshape(deep, occ).astype(jnp.float32)
        return direct, lprime

    def put(step, direct, lprime):
        turned = direct.T.astype(jnp.bfloat16)
        sent[:, step, :, 0:wide] = turned.reshape(n, rows, wide)
        turned = lprime.T.astype(jnp.bfloat16)
        sent[:, step, :, wide:span] = turned.reshape(n, rows, deep)
        got[me, step] = sent[me, step]

    def send(k):
        for peer in peers:
            message(k, peer).start()

    half_whole = whole_virt // 2

    def half_form(part, which, direct, lprime):
        part = pl.ds(pl.multiple_of(part * half_whole, 128), half_whole)
        block = amps_t[part, columns_of(which)]
        vv = vv_buf[0, :, :, part].reshape(wide, half_whole)
        ov = ov_buf[0, :, :, part].reshape(deep, half_whole)
        direct = direct + jnp.dot(vv, block, preferred_element_type=jnp.float32)
        lprime = lprime + jnp.dot(ov, block, preferred_element_type=jnp.float32)
        return direct, lprime

    def start_form(which):
        direct = vo_buf[0, :, :, columns_of(which)].reshape(wide, half_occ).astype(jnp.float32)
        lprime = oo_buf[0, :, :, columns_of(which)].reshape(deep, half_occ).astype(jnp.float32)
        return half_form(side, which, direct, lprime)

    def put_half(which, direct, lprime):
        part = pl.ds(which * half_n, half_n)
        turned = direct.T.astype(jnp.bfloat16)
        sent[part, 0, :, 0:wide] = turned.reshape(half_n, rows, wide)
        turned = lprime.T.astype(jnp.bfloat16)
        sent[part, 0, :, wide:span] = turned.reshape(half_n, rows, deep)

    greet_partner(mate)
    pass_on(home, 0, False)
    for peer in targets:
        hop(me, 1, peer // half_n, peer).start()
    pass_on(cross, 0, True)
    for copy in loads(0, 0):
        copy.wait()
    close(home, 0)
    direct, lprime = start_form(other)
    close(cross, 0)
    direct, lprime = half_form(other, other, direct, lprime)
    put_half(other, direct, lprime)
    for peer in cross[quarter_n:]:
        greet(peer)
    for peer in cross:
        message(0, peer).start()
    pass_on(home, 1, False)
    pass_on(cross, 1, True)
    close(home + cross, 1)
    direct, lprime = start_form(side)
    direct, lprime = half_form(other, side, direct, lprime)
    put_half(side, direct, lprime)
    got[me, 0] = sent[me, 0]
    for peer in home:
        message(0, peer).start()
    for partner in partners[1:]:
        greet_partner(partner)

    @pl.when(is_near)
    def _():
        ref = amps_t
        remote(ref, ref, gather_send, gather_recv.at[0, me], {"pb": mate}).wait_send()

    @pl.when(jnp.logical_not(is_near))
    def _():
        ref = amps_t.at[pl.ds(0, (n - 2) * virt), :]
        remote(ref, ref, gather_send, gather_recv.at[0, me], {"pb": mate}).wait_send()

    for s in range(n):
        block = amps_t[s * virt:(s + 1) * virt, :]
        amps_t_f32 = block.astype(jnp.float32)
        tiled[:, s * virt:(s + 1) * virt] = amps_t_f32.T
    for s in range(n):
        part = tiled[s * rows:(s + 1) * rows, :].astype(jnp.bfloat16)
        for q in range(group):
            amps[s * deep + q * rows:s * deep + (q + 1) * rows, :] = part
    own_rows = amps[pl.ds(pl.multiple_of(me * deep, 128), rows), :]
    gram[...] = jnp.dot(own_rows, amps_t[...], preferred_element_type=jnp.float32)
    coul_sent[...] = jnp.zeros_like(coul_sent)

    def produce(step, carry):
        slot = lax.rem(step, 2)

        @pl.when(step + 1 < steps)
        def _():
            for copy in loads(step + 1, 1 - slot):
                copy.start()

        @pl.when(step > 0)
        def _():
            for copy in loads(step, slot):
                copy.wait()

        direct, lprime = form(slot)

        @pl.when(step > 0)
        def _():
            put(step, direct, lprime)

        own_amps = amps_t[own_block, :].astype(jnp.float32)
        lane = lax.broadcasted_iota(jnp.int32, coul_sent.shape, 1)
        held = coul_sent[...]
        for q in range(group):
            from_direct = direct[q * virt:(q + 1) * virt] * own_amps
            from_occ = lprime[q * rows:(q + 1) * rows] * gram[...]
            value = jnp.sum(from_direct) - jnp.sum(from_occ)
            held = jnp.where(lane == step * group + q, value, held)
        coul_sent[...] = held

        for k in range(1, early):
            @pl.when(step == k)
            def _():
                send(k)

        return carry

    lax.fori_loop(0, steps, produce, 0)

    for d in range(n - 1):
        remote(coul_sent, coul_got.at[me], coul_sem.at[0], coul_sem.at[1], {"pq": peers[d]}).start()
    for k, (first, count) in enumerate(chunks):
        if early <= first < middle:
            send(k)
    all_coul = coul_got.at[pl.ds(0, n - 1)]
    remote(all_coul, all_coul, coul_sem.at[0], coul_sem.at[1], {"pq": peers[0]}).wait()

    coulomb = coul_sent[...]
    for d in range(n - 1):
        coulomb = coulomb + coul_got[peers[d]]
    lines = -(-steps // 8) * 8
    spread = jnp.broadcast_to(coulomb, (lines, 128))
    lane = lax.broadcasted_iota(jnp.int32, (lines, 128), 1)
    first = lax.broadcasted_iota(jnp.int32, (lines, 128), 0) * group
    spread = jnp.where((lane >= first) & (lane < first + group), spread, 0.0)
    column = lax.broadcasted_iota(jnp.int32, (128, span), 1)
    vector = jnp.zeros((128, span), jnp.int32)
    for q in range(1, group):
        vector = vector + jnp.where((column >= q * virt) & (column < wide), 1, 0)
        vector = vector + jnp.where(column >= wide + q * rows, 1, 0)
    place_of = lax.rem(lax.broadcasted_iota(jnp.int32, (128, span), 0), group)
    pick = jnp.where(place_of == vector, 1.0, 0.0)
    weights = jnp.dot(
        spread, pick, preferred_element_type=jnp.float32, precision=lax.Precision.HIGHEST
    )

    def weigh(d, carry):
        total = jnp.zeros((rows, span), jnp.float32)
        for s in range(steps):
            total = total + weights[s:s + 1, :] * sent[d, s].astype(jnp.float32)
        from_direct = total[:, 0:virt]
        from_occ = total[:, wide:wide + rows]
        for q in range(1, group):
            from_direct = from_direct + total[:, q * virt:(q + 1) * virt]
            from_occ = from_occ + total[:, wide + q * rows:wide + (q + 1) * rows]
        total = jnp.concatenate([from_direct, from_occ], axis=1)
        for m in range(n_pb):
            part_sent[m, d] = total[m * sub:(m + 1) * sub]
        return carry

    lax.fori_loop(0, n, weigh, 0)

    for partner in partners:
        remote(
            part_sent.at[partner], part_got.at[mine], part_sem.at[0], part_sem.at[1], {"pb": partner}
        ).start()

    def consume(step, carry):
        @pl.when(step == min(2, last - 1))
        def _():
            three = part_got.at[pl.ds(0, n_pb - 1)]
            remote(three, three, part_sem.at[0], part_sem.at[1], {"pb": mate}).wait()
            total = part_sent[mine]
            for partner in partners:
                total = total + part_got[partner]
            total = total.astype(jnp.bfloat16)
            for s in range(n):
                sums_sent[s] = jnp.concatenate([total[s, :, 0:128], total[s, :, 128:256]], axis=0)
            sums_got[me] = sums_sent[me]
            for d in range(n - 1):
                remote(
                    sums_sent.at[peers[d]], sums_got.at[me], sums_sem.at[0], sums_sem.at[1],
                    {"pq": peers[d]},
                ).start()
            for k, (first, count) in enumerate(chunks):
                if first >= middle:
                    send(k)
            for peer in peers:
                last_message(peer, lprime_columns, 0).start()
            for peer in peers:
                last_message(peer, direct_columns, 1).start()

        @pl.when(step == last - 1)
        def _():
            several = sums_got.at[pl.ds(0, n - 1)]
            remote(several, several, sums_sem.at[0], sums_sem.at[1], {"pq": peers[0]}).wait()
            pieces = [sums_got[s] for s in range(n)]
            pieces = [
                jnp.concatenate([piece[0:sub], piece[sub:2 * sub]], axis=1).astype(jnp.float32)
                for piece in pieces
            ]
            partial_sum = jnp.concatenate([piece[:, 0:virt] for piece in pieces], axis=1)
            from_occ = jnp.concatenate([piece[:, virt:virt + rows] for piece in pieces], axis=1)
            from_occ = jnp.dot(
                from_occ.astype(jnp.bfloat16), tiled[...].astype(jnp.bfloat16),
                preferred_element_type=jnp.float32,
            )
            strip = pl.ds(pl.multiple_of(mine * sub, 8), sub)
            fock_ref[strip, :] = (partial_sum - from_occ) * (2.0 / (batch * n_pb))
            for partner in partners:
                remote(
                    fock_ref.at[strip], fock_ref.at[strip], fock_sem.at[0], fock_sem.at[1],
                    {"pb": partner},
                ).start()

        for k, (first, count) in enumerate(chunks):
            @pl.when(step == first)
            def _():
                ref = got.at[pl.ds(0, n - 1), pl.ds(first, count)]
                arrived(ref, recv_sem.at[k], {"pq": peers[0]})

        subtract(step)
        finish(step)
        return carry

    def subtract(step):
        lane_q = lax.broadcasted_iota(jnp.int32, (rows, deep), 1) // rows
        columns = []
        for s in range(n):
            piece = got[s, step, :, wide:span]
            columns.append(jnp.concatenate(
                [jnp.where(lane_q == q, piece, jnp.zeros_like(piece)) for q in range(group)], axis=0
            ))
        occ_buf[...] = jnp.dot(
            jnp.concatenate(columns, axis=1), amps[...], preferred_element_type=jnp.float32
        )

    def finish(step):
        for q in range(group):
            dressed[step * group + q] = finished(n, virt, rows, got, occ_buf, step, q)

    lax.fori_loop(0, last, consume, 0)
    ref = got.at[pl.ds(0, n - 1), last, :, lprime_columns]
    arrived(ref, recv_sem.at[len(chunks)], {"pq": peers[0]})
    subtract(last)
    strips = fock_ref.at[pl.ds(0, (n_pb - 1) * sub)]
    remote(strips, strips, fock_sem.at[0], fock_sem.at[1], {"pb": mate}).wait()
    everything = sent.at[pl.ds(0, n - 1)]
    remote(everything, everything, send_sem, recv_sem.at[0], {"pq": peers[0]}).wait_send()
    ref = got.at[pl.ds(0, n - 1), last, :, direct_columns]
    arrived(ref, recv_sem.at[len(chunks) + 1], {"pq": peers[0]})


def finished(n, virt, rows, got, occ_buf, step, q):
    partial_sum = jnp.concatenate(
        [got[s, step, :, q * virt:(q + 1) * virt].astype(jnp.float32) for s in range(n)], axis=1
    )
    return (partial_sum - occ_buf[q * rows:(q + 1) * rows, :]).astype(jnp.bfloat16)


def store(n, virt, group, dressed, fock, got, occ_buf, dressed_out, fock_out, tail, sems):
    batch, rows = dressed.shape[:2]
    done = batch - group
    parts = 2
    size = done // parts
    copies = [
        pltpu.make_async_copy(
            dressed.at[pl.ds(p * size, size)], dressed_out.at[pl.ds(p * size, size)], sems.at[p]
        )
        for p in range(parts)
    ]
    copies.append(pltpu.make_async_copy(fock, fock_out, sems.at[parts]))
    for copy in copies:
        copy.start()
    for q in range(group):
        tail[q] = finished(n, virt, rows, got, occ_buf, batch // group - 1, q)
    copies.append(
        pltpu.make_async_copy(tail, dressed_out.at[pl.ds(done, group)], sems.at[parts + 1])
    )
    copies[-1].start()
    for copy in copies:
        copy.wait()


def fused(n, n_pb, group, chol_vv, chol_ov, chol_oo, chol_vo, amplitudes):
    batch, virt, whole_virt = chol_vv.shape
    rows, occ = chol_ov.shape[1], chol_oo.shape[2]
    steps = batch // group
    wide, deep = group * virt, group * rows
    sub = rows // n_pb
    bf16, f32 = jnp.bfloat16, jnp.float32
    dma = pltpu.SemaphoreType.DMA
    whole = pl.BlockSpec(memory_space=pltpu.VMEM)
    hbm = pl.BlockSpec(memory_space=pl.ANY)
    dressed, fock, got, occupied = pl.pallas_call(
        functools.partial(kernel, n, n_pb, group),
        out_shape=(
            pltpu.VMEM((batch, rows, whole_virt), bf16),
            pltpu.VMEM((rows, whole_virt), f32),
            pltpu.VMEM((n, steps, rows, wide + deep), bf16),
            pltpu.VMEM((deep, whole_virt), f32),
        ),
        in_specs=[hbm, hbm, hbm, hbm, hbm],
        out_specs=(whole, whole, whole, whole),
        scratch_shapes=[
            pltpu.VMEM((2, group, virt, whole_virt), bf16),
            pltpu.VMEM((2, group, rows, whole_virt), bf16),
            pltpu.VMEM((2, group, rows, occ), bf16),
            pltpu.VMEM((2, group, virt, occ), bf16),
            pltpu.VMEM((whole_virt, occ), bf16),
            pltpu.VMEM((n * deep, whole_virt), bf16),
            pltpu.VMEM((occ, whole_virt), f32),
            pltpu.VMEM((rows, occ), f32),
            pltpu.VMEM((n, steps, rows, wide + deep), bf16),
            pltpu.VMEM((1, 128), f32),
            pltpu.VMEM((n, 1, 128), f32),
            pltpu.VMEM((n_pb, n, sub, virt + rows), f32),
            pltpu.VMEM((n_pb, n, sub, virt + rows), f32),
            pltpu.VMEM((n, 2 * sub, 128), bf16),
            pltpu.VMEM((n, 2 * sub, 128), bf16),
            dma((2, 4)), dma, dma, dma((4, n)), dma, dma((13,)),
            dma((2,)), dma((2,)), dma((2,)), dma((2,)),
            pltpu.SemaphoreType.REGULAR((n + n_pb,)),
        ],
        compiler_params=pltpu.CompilerParams(
            collective_id=0, has_side_effects=True, vmem_limit_bytes=48 * 1024 * 1024
        ),
    )(chol_vv, chol_ov, chol_oo, jnp.swapaxes(chol_vo, 1, 2), amplitudes.T)
    return pl.pallas_call(
        functools.partial(store, n, virt, group),
        out_shape=(
            jax.ShapeDtypeStruct(dressed.shape, bf16),
            jax.ShapeDtypeStruct(fock.shape, f32),
        ),
        in_specs=[whole, whole, whole, whole],
        out_specs=(hbm, hbm),
        scratch_shapes=[pltpu.VMEM((group, rows, whole_virt), bf16), dma((4,))],
        compiler_params=pltpu.CompilerParams(vmem_limit_bytes=8 * 1024 * 1024),
    )(dressed, fock, got, occupied)


def group_size(batch, virt, rows):
    for group in range(1, batch + 1):
        if batch % group == 0 and group * virt % 128 == 0 and group * rows % 128 == 0:
            return group
    return None


def solution(mesh):
    n, n_pb = mesh.shape["pq"], mesh.shape["pb"]
    in_specs = (
        P("pb", "pq", None),
        P("pb", "pq", None),
        P("pb", "pq", None),
        P("pb", None, "pq"),
        P(None, "pq"),
    )
    out_specs = (P("pb", "pq", None), P("pq", None))

    def body(chol_vv, chol_ov, chol_oo, chol_vo, amplitudes):
        batch, virt, whole_virt = chol_vv.shape
        rows, occ = chol_ov.shape[1], chol_oo.shape[2]
        group = group_size(batch, virt, rows)
        fits = group is not None and group <= 8 and virt % 32 == 0 and rows % 16 == 0
        fits = fits and occ % 256 == 0 and n_pb == 4 and n == 8
        fits = fits and virt + rows == 256 and rows == 8 * n_pb and 3 <= batch // group <= 16
        fits = fits and batch <= 128 and whole_virt % 256 == 0
        if fits:
            return fused(n, n_pb, group, chol_vv, chol_ov, chol_oo, chol_vo, amplitudes)
        return per_device(chol_vv, chol_ov, chol_oo, chol_vo, amplitudes)

    return jax.shard_map(
        body, mesh=mesh, in_specs=in_specs, out_specs=out_specs, check_vma=False
    )
```
